256 devices in a mesh: seq: 128 (over y_hi, x, z, core), dp: 2 (over y_lo).
Axes of the slice: x: 4, y: 4 (y_hi: 2, y_lo: 2; y = y_hi * 2 + y_lo), z: 8, core: 2. Of those that a mesh axis runs over, the one named last changes fastest.
Arguments:
- spectrum: bfloat16 [128, 64, 2, 1025], P('seq', 'dp'), parts along dimension 1, may hold values from -6 to 6
- band_table: int32 [60, 2], replicated, may hold values from 0 to 1024, as said below
- band_weight: bfloat16 [60, 2, 64, 384], replicated, may hold values from -0.5 to 0.5
- qkv_weight: bfloat16 [2, 384, 1152], replicated, may hold values from -1.5 to 1.5
- out_weight: bfloat16 [2, 384, 384], replicated, may hold values from -0.3125 to 0.3125
- ff_in_weight: bfloat16 [2, 384, 768], replicated, may hold values from -0.3125 to 0.3125
- ff_out_weight: bfloat16 [2, 768, 384], replicated, may hold values from -0.21875 to 0.21875
- norm_gains: float32 [6, 384], replicated, may hold values from 0.1 to 1.9
Outputs:
- hidden_out: bfloat16 [128, 64, 60, 384], P('seq', 'dp'), parts along dimension 1
The draws below stay inside these ranges and needn't reach their ends.
There are 2 independent parts, one for each index of `dp`. The reference program is written for one: setup_inputs(seed, part) draws one part's arguments, and reference() takes and returns one part's arrays. A program takes and returns all parts, laid end to end along the dimension named above; an argument that names none is the same for every part. Nothing has to cross between parts.
Inputs may be any that keep to these rules, and one draw needn't show every extreme that they name: `band_table`: row n holds band n's first bin and its number of bins; each band lies inside the 1025 bins and has 2 to 64 bins, the last band exactly 64; bands intersect at low frequencies.
All inputs are finite; a program needn't handle non-finite values.
Results may differ from the reference program's by a relative error of at most 0.017.
Values may be sent and summed in bfloat16 or wider, within the bound.
A program may use at most 128 MiB of HBM per device.

```python
import math
import jax
import jax.numpy as jnp
from jax import lax

D = 384
HEADS = 8
BANDS = 60
BINS = 1025
SPAN = 64
CH = 2
FFH = 768
BATCH = 32
FRAMES = 128


def draw_band_table(key, part):
    first_key = jax.random.fold_in(key, 11)
    second_key = jax.random.fold_in(key, 23)
    index = jnp.arange(BANDS, dtype=jnp.int32)
    lower = 4 + (SPAN - 4) * index // (BANDS - 1)
    shrink = jax.random.randint(first_key, (BANDS,), 0, 1 << 20) % (lower // 2 + 1)
    widths = lower - shrink
    widths = jnp.where(index == BANDS - 1, SPAN, widths).astype(jnp.int32)
    base = (BINS - SPAN) * index * index // ((BANDS - 1) * (BANDS - 1))
    jitter = jax.random.randint(second_key, (BANDS,), 0, 4)
    starts = jnp.minimum(base + jitter, BINS - widths).astype(jnp.int32)
    return jnp.stack([starts, widths], axis=1).astype(jnp.int32)


def draw_qkv_weight(key, part):
    base = jax.random.normal(jax.random.fold_in(key, 5), (2, D, 3 * D), jnp.float32) * D ** (-0.5)
    return jnp.clip(base, -1.5, 1.5).astype(jnp.bfloat16)


def shard_levels(rng, extent, cuts, least, largest):
    def one(position, blocks):
        draws = jax.random.uniform(jax.random.fold_in(jax.random.fold_in(rng, 6), position), (blocks,), jnp.float32, least / len(cuts), largest / len(cuts))
        return jnp.repeat(jnp.exp(draws), extent[position] // blocks).reshape((-1,) + (1,) * (len(extent) - position - 1))

    gain = one(*cuts[0])
    for cut in cuts[1:]:
        gain = gain * one(*cut)
    return gain


def gaussian(key, dims, spread, most, pieces=(), kind=jnp.bfloat16):
    result = spread * jax.random.normal(key, dims, jnp.float32)
    if pieces:
        result = result * shard_levels(key, dims, pieces, -0.22, 0.18)
    return jnp.clip(result, -most, most).astype(kind)


def setup_inputs(seed: int = 0, part: int = 0) -> dict:
    arg_keys = jax.random.split(jax.random.key(seed), 9)
    part_keys = jax.random.split(jax.random.fold_in(arg_keys[8], part), 9)
    spectrum = gaussian(part_keys[0], (FRAMES, BATCH, CH, BINS), 1.0, 6.0, ((0, 128),))
    band_table = draw_band_table(jax.random.fold_in(arg_keys[8], 71), part)
    band_weight = gaussian(arg_keys[2], (BANDS, CH, SPAN, D), (CH * SPAN) ** -0.5, 0.5)
    qkv_weight = draw_qkv_weight(jax.random.fold_in(arg_keys[8], 71), part)
    out_weight = gaussian(arg_keys[4], (2, D, D), D ** -0.5, 0.3125)
    ff_in_weight = gaussian(arg_keys[5], (2, D, FFH), D ** -0.5, 0.3125)
    ff_out_weight = gaussian(arg_keys[6], (2, FFH, D), FFH ** -0.5, 0.21875)
    norm_gains = jnp.clip(1.0 + 0.18 * jax.random.normal(arg_keys[7], (6, D), jnp.float32), 0.1, 1.9)
    return dict(spectrum=spectrum, band_table=band_table, band_weight=band_weight, qkv_weight=qkv_weight, out_weight=out_weight, ff_in_weight=ff_in_weight, ff_out_weight=ff_out_weight, norm_gains=norm_gains)


EPSILON = 0.05

def normalize(values, gain_row):
    return values * lax.rsqrt(lax.optimization_barrier(jnp.mean(values * values, axis=-1, keepdims=True)) + EPSILON) * gain_row

def rotate(tensor, positions):
    half_size = tensor.shape[-1] // 2
    frequency = 10000.0 ** (-jnp.arange(half_size, dtype=jnp.float32) / half_size)
    angles = positions[..., None] * frequency
    cosine = jnp.cos(angles)
    sine_part = jnp.sin(angles)
    first_half = tensor[..., :half_size]
    second_half = tensor[..., half_size:]
    return jnp.concatenate([first_half * cosine - second_half * sine_part, second_half * cosine + first_half * sine_part], axis=-1)

def project(stream, weights, gain_row, positions):
    normed = normalize(stream.astype(jnp.float32), gain_row).astype(jnp.bfloat16)
    mixture = jnp.dot(normed, weights, preferred_element_type=jnp.float32)
    model_width = stream.shape[-1]
    head_shape = stream.shape[:-1] + (HEADS, model_width // HEADS)
    queries = rotate(mixture[..., :model_width].reshape(head_shape), positions).astype(jnp.bfloat16).reshape(stream.shape)
    key_rows = rotate(mixture[..., model_width:2 * model_width].reshape(head_shape), positions).astype(jnp.bfloat16).reshape(stream.shape)
    value_rows = mixture[..., 2 * model_width:].astype(jnp.bfloat16)
    return (queries, key_rows, value_rows)

def attend_rows(queries, key_rows, value_rows):
    row_count, length, model_width = queries.shape
    head_size = model_width // HEADS
    head_shape = (row_count, length, HEADS, head_size)
    scores = jnp.einsum('rshd,rthd->rhst', queries.reshape(head_shape).astype(jnp.float32), key_rows.reshape(head_shape).astype(jnp.float32)) / math.sqrt(head_size)
    weights = jax.nn.softmax(scores, axis=-1).astype(jnp.bfloat16)
    context = jnp.einsum('rhst,rthd->rshd', weights.astype(jnp.float32), value_rows.reshape(head_shape).astype(jnp.float32))
    return context.astype(jnp.bfloat16).reshape(row_count, length, model_width)

def attend_time(queries, key_rows, value_rows):
    swapped = (jnp.swapaxes(queries, 0, 1), jnp.swapaxes(key_rows, 0, 1), jnp.swapaxes(value_rows, 0, 1))

    def single(triple):
        return attend_rows(triple[0][None], triple[1][None], triple[2][None])[0]
    return jnp.swapaxes(lax.map(single, swapped), 0, 1)

def finish(stream, context, weights):
    return (stream.astype(jnp.float32) + jnp.dot(context, weights, preferred_element_type=jnp.float32)).astype(jnp.bfloat16)

def feed_forward(stream, weight_in, weight_out, gain_row):
    normed = normalize(stream.astype(jnp.float32), gain_row).astype(jnp.bfloat16)
    active = jax.nn.gelu(jnp.dot(normed, weight_in, preferred_element_type=jnp.float32), approximate=True).astype(jnp.bfloat16)
    return (stream.astype(jnp.float32) + jnp.dot(active, weight_out, preferred_element_type=jnp.float32)).astype(jnp.bfloat16)

def reference(spectrum, band_table, band_weight, qkv_weight, out_weight, ff_in_weight, ff_out_weight, norm_gains):
    offsets = jnp.arange(SPAN, dtype=jnp.int32)
    targets = (band_table[:, 0:1] + offsets[None, :]).astype(jnp.int32)
    valid = offsets[None, :] < band_table[:, 1:2]
    picked = jnp.take(spectrum, targets.reshape(-1), axis=3).reshape(FRAMES, BATCH, CH, BANDS, SPAN)
    picked = jnp.where(valid[None, None, None], picked, jnp.zeros((), picked.dtype))
    embedded = jnp.einsum('fbcnj,ncjd->fbnd', picked.astype(jnp.float32), band_weight.astype(jnp.float32))
    stream = normalize(embedded, norm_gains[0]).astype(jnp.bfloat16)
    band_positions = jnp.arange(BANDS, dtype=jnp.float32).reshape(1, BANDS, 1)

    def band_layer(block):
        triple = project(block, qkv_weight[0], norm_gains[1], band_positions)
        mixed_block = finish(block, attend_rows(triple[0], triple[1], triple[2]), out_weight[0])
        return feed_forward(mixed_block, ff_in_weight[0], ff_out_weight[0], norm_gains[2])
    stream = lax.map(band_layer, stream)
    frame_positions = jnp.arange(FRAMES, dtype=jnp.float32).reshape(FRAMES, 1, 1)

    def time_layer(block):
        triple = project(block, qkv_weight[1], norm_gains[3], frame_positions)
        mixed_block = finish(block, attend_time(triple[0], triple[1], triple[2]), out_weight[1])
        return feed_forward(mixed_block, ff_in_weight[1], ff_out_weight[1], norm_gains[4])
    by_batch = lax.map(time_layer, jnp.swapaxes(stream, 0, 1))
    stream = jnp.swapaxes(by_batch, 0, 1)
    return normalize(stream.astype(jnp.float32), norm_gains[5]).astype(jnp.bfloat16)
```

```python
import functools
import math

import jax
import jax.numpy as jnp
from jax import lax
from jax.experimental import pallas as pl
from jax.experimental.pallas import tpu as pltpu
from jax.sharding import PartitionSpec as P

HEADS = 8
SPAN = 64


EPSILON = 0.05


def normalize(values, gain_row):
    return (
        values * lax.rsqrt(jnp.mean(values * values, axis=-1, keepdims=True) + EPSILON) * gain_row
    )


def rotate(tensor, positions):
    half_size = tensor.shape[-1] // 2
    frequency = 10000.0 ** (-jnp.arange(half_size, dtype=jnp.float32) / half_size)
    angles = positions[..., None] * frequency
    cosine = jnp.cos(angles)
    sine_part = jnp.sin(angles)
    first_half = tensor[..., :half_size]
    second_half = tensor[..., half_size:]
    return jnp.concatenate(
        [
            first_half * cosine - second_half * sine_part,
            second_half * cosine + first_half * sine_part,
        ],
        axis=-1,
    )


def project(stream, weights, gain_row, positions):
    normed = normalize(stream.astype(jnp.float32), gain_row).astype(jnp.bfloat16)
    mixture = jnp.dot(normed, weights, preferred_element_type=jnp.float32)
    model_width = stream.shape[-1]
    head_shape = stream.shape[:-1] + (HEADS, model_width // HEADS)
    queries = (
        rotate(mixture[..., :model_width].reshape(head_shape), positions)
        .astype(jnp.bfloat16)
        .reshape(stream.shape)
    )
    key_rows = (
        rotate(mixture[..., model_width : 2 * model_width].reshape(head_shape), positions)
        .astype(jnp.bfloat16)
        .reshape(stream.shape)
    )
    value_rows = mixture[..., 2 * model_width :].astype(jnp.bfloat16)
    return (queries, key_rows, value_rows)


def attend_rows(queries, key_rows, value_rows):
    row_count, length, model_width = queries.shape
    head_size = model_width // HEADS
    head_shape = (row_count, length, HEADS, head_size)
    scores = jnp.einsum(
        "rshd,rthd->rhst",
        queries.reshape(head_shape),
        key_rows.reshape(head_shape),
        preferred_element_type=jnp.float32,
    ) / math.sqrt(head_size)
    weights = jax.nn.softmax(scores, axis=-1).astype(jnp.bfloat16)
    context = jnp.einsum(
        "rhst,rthd->rshd",
        weights,
        value_rows.reshape(head_shape),
        preferred_element_type=jnp.float32,
    )
    return context.astype(jnp.bfloat16).reshape(row_count, length, model_width)


def attend_time(queries, key_rows, value_rows):
    context = attend_rows(
        jnp.swapaxes(queries, 0, 1), jnp.swapaxes(key_rows, 0, 1), jnp.swapaxes(value_rows, 0, 1)
    )
    return jnp.swapaxes(context, 0, 1)


def finish(stream, context, weights):
    return (
        stream.astype(jnp.float32) + jnp.dot(context, weights, preferred_element_type=jnp.float32)
    ).astype(jnp.bfloat16)


def feed_forward(stream, weight_in, weight_out, gain_row):
    normed = normalize(stream.astype(jnp.float32), gain_row).astype(jnp.bfloat16)
    active = jax.nn.gelu(
        jnp.dot(normed, weight_in, preferred_element_type=jnp.float32), approximate=True
    ).astype(jnp.bfloat16)
    return (
        stream.astype(jnp.float32) + jnp.dot(active, weight_out, preferred_element_type=jnp.float32)
    ).astype(jnp.bfloat16)


def flatten_items(block):
    return block.reshape(block.shape[0], block.shape[2], block.shape[3])


def exchange_kernel(groups, block_ref, out_ref, send_sem, recv_sem):
    me = lax.axis_index("seq")
    barrier = pltpu.get_barrier_semaphore()

    def greet(step, carry):
        pl.semaphore_signal(
            barrier,
            inc=1,
            device_id={"seq": lax.rem(me + step, groups)},
            device_id_type=pl.DeviceIdType.MESH,
        )
        return carry

    lax.fori_loop(1, groups, greet, 0)
    pl.semaphore_wait(barrier, groups - 1)

    def send(step, carry):
        target = lax.rem(me + step, groups)
        pltpu.make_async_remote_copy(
            src_ref=block_ref.at[target],
            dst_ref=out_ref.at[me],
            send_sem=send_sem,
            recv_sem=recv_sem,
            device_id={"seq": target},
            device_id_type=pl.DeviceIdType.MESH,
        ).start()
        return carry

    lax.fori_loop(1, groups, send, 0)
    own = pltpu.make_async_copy(block_ref.at[me], out_ref.at[me], recv_sem)
    own.start()
    pltpu.make_async_copy(out_ref, out_ref, recv_sem).wait()
    sent = block_ref.at[pl.ds(0, groups - 1)]
    pltpu.make_async_copy(sent, sent, send_sem).wait()


def exchange(block, collective_id):
    groups = block.shape[0]
    return pl.pallas_call(
        functools.partial(exchange_kernel, groups),
        out_shape=jax.ShapeDtypeStruct(block.shape, block.dtype),
        in_specs=[pl.BlockSpec(memory_space=pltpu.VMEM)],
        out_specs=pl.BlockSpec(memory_space=pltpu.VMEM),
        scratch_shapes=[pltpu.SemaphoreType.DMA(()), pltpu.SemaphoreType.DMA(())],
        compiler_params=pltpu.CompilerParams(collective_id=collective_id, has_side_effects=True),
    )(block)


def body(
    spectrum,
    band_table,
    band_weight,
    qkv_weight,
    out_weight,
    ff_in_weight,
    ff_out_weight,
    norm_gains,
):
    frame_count, batch_size, channel_count, bin_count = spectrum.shape
    band_count = band_table.shape[0]
    offsets = jnp.arange(SPAN, dtype=jnp.int32)
    targets = (band_table[:, 0:1] + offsets[None, :]).reshape(-1)
    valid = (offsets[None, :] < band_table[:, 1:2]).reshape(-1)
    chosen = (
        (jnp.arange(bin_count, dtype=jnp.int32)[:, None] == targets[None, :]) & valid[None, :]
    ).astype(jnp.bfloat16)
    features = jnp.einsum(
        "fbcq,qm->fbcm", spectrum, chosen, preferred_element_type=jnp.float32
    ).astype(jnp.bfloat16)
    features = features.reshape(frame_count, batch_size, channel_count, band_count, SPAN)
    embedded = jnp.einsum(
        "fbcnj,ncjd->fbnd", features, band_weight, preferred_element_type=jnp.float32
    )
    model_width = embedded.shape[-1]
    stream = normalize(embedded, norm_gains[0]).astype(jnp.bfloat16)
    stream = stream.reshape(frame_count * batch_size, band_count, model_width)
    band_positions = jnp.arange(band_count, dtype=jnp.float32).reshape(1, band_count, 1)
    triple = project(stream, qkv_weight[0], norm_gains[1], band_positions)
    stream = finish(stream, attend_rows(triple[0], triple[1], triple[2]), out_weight[0])
    stream = feed_forward(stream, ff_in_weight[0], ff_out_weight[0], norm_gains[2])
    groups = lax.axis_size("seq")
    pair_count = batch_size * band_count
    per_group = pair_count // groups
    stream = stream.reshape(groups, per_group, model_width)
    stream = jnp.pad(stream, ((0, 0), (0, 1), (0, 0)))
    flat = exchange(stream, 0)[:, :per_group]
    length = flat.shape[0]
    frame_positions = jnp.arange(length, dtype=jnp.float32).reshape(length, 1, 1)
    parts = project(flat, qkv_weight[1], norm_gains[3], frame_positions)
    mixed_block = finish(flat, attend_time(parts[0], parts[1], parts[2]), out_weight[1])
    result_block = feed_forward(mixed_block, ff_in_weight[1], ff_out_weight[1], norm_gains[4])
    regrouped = jnp.pad(result_block, ((0, 0), (0, 1), (0, 0)))
    stream = exchange(regrouped, 1)[:, :per_group]
    stream = stream.reshape(frame_count, pair_count, model_width)
    result = normalize(stream.astype(jnp.float32), norm_gains[5]).astype(jnp.bfloat16)
    return result.reshape(frame_count, batch_size, band_count, model_width)


def solution(mesh):
    in_specs = (P("seq", "dp", None, None), P(), P(), P(), P(), P(), P(), P())
    out_specs = P("seq", "dp", None, None)
    return jax.shard_map(body, mesh=mesh, in_specs=in_specs, out_specs=out_specs, check_vma=False)
```

```python
import functools
import math

import jax
import jax.numpy as jnp
import numpy as np
from jax import lax
from jax.experimental import pallas as pl
from jax.experimental.pallas import tpu as pltpu
from jax.sharding import PartitionSpec as P

D = 384
HEADS = 8
HEAD = 48
HALF = 24
SPAN = 64
EPSILON = 0.05
WIDE = 512
CHUNK = 8
SLOTS = 64
TILE = 256
NEG = -1e30
MESH = pl.DeviceIdType.MESH


def head_columns():
    rotary = np.zeros((D, WIDE), np.float32)
    value = np.zeros((D, WIDE), np.float32)
    for head in range(HEADS):
        base = (head // 2) * 128
        for i in range(HEAD):
            half, j = divmod(i, HALF)
            rotary[head * HEAD + i, base + 64 * half + (head % 2) * HALF + j] = 1
            value[head * HEAD + i, base + 64 * (head % 2) + i] = 1
    return rotary, value


def rotary_tables(positions):
    frequency = 10000.0 ** (-np.arange(HALF, dtype=np.float64) / HALF)
    angles = positions[:, None].astype(np.float64) * frequency
    cosine = np.zeros((len(positions), 128))
    sine = np.zeros((len(positions), 128))
    for head in range(2):
        for half in range(2):
            at = 64 * half + head * HALF
            cosine[:, at : at + HALF] = np.cos(angles)
            sine[:, at : at + HALF] = np.sin(angles) * (1 if half else -1)
    scale = math.log2(math.e) / math.sqrt(HEAD)
    return [cosine * scale, sine * scale, cosine, sine]


def swap_matrix(outer, inner):
    result = np.zeros((outer * inner, outer * inner), np.float32)
    for i in range(outer):
        for j in range(inner):
            result[j * outer + i, i * inner + j] = 1
    return result


def normalize(values, gain):
    return (
        values
        * lax.rsqrt(jnp.mean(values * values, axis=-1, keepdims=True) + EPSILON)
        * gain
    )


def dot(a, b):
    return jnp.dot(a, b, preferred_element_type=jnp.float32)


def kernel(
    groups,
    bands,
    table,
    spectrum,
    gains,
    band_hbm,
    qkv_hbm,
    mix_hbm,
    ff_in_hbm,
    ff_out_hbm,
    rope_hbm,
    rotary_hbm,
    value_hbm,
    spread_hbm,
    swap_hbm,
    out_ref,
    band_w,
    qkv_raw,
    mix_raw,
    ff_in,
    ff_out,
    rope,
    rotary_p,
    value_p,
    spread_p,
    swap_p,
    qkv_w,
    mix_w,
    embedded,
    stream,
    arrived,
    turned,
    hidden,
    leaving,
    q_s,
    k_s,
    v_s,
    c_s,
    lanes,
    load_sem,
    send_sem,
    recv_sem,
):
    me = lax.axis_index("seq")
    half_rows = groups * CHUNK
    quarter = bands // 4

    loads = [
        pltpu.make_async_copy(src, dst, load_sem.at[i])
        for i, (src, dst) in enumerate(
            [
                (rotary_hbm, rotary_p),
                (value_hbm, value_p),
                (qkv_hbm, qkv_raw),
                (spread_hbm, spread_p),
                (mix_hbm, mix_raw),
            ]
            + [
                (
                    band_hbm.at[pl.ds(i * quarter, quarter)],
                    band_w.at[pl.ds(i * quarter, quarter)],
                )
                for i in range(4)
            ]
            + [
                (swap_hbm, swap_p),
                (rope_hbm, rope),
                (ff_in_hbm, ff_in),
                (ff_out_hbm, ff_out),
            ]
        )
    ]
    for load in loads:
        load.start()

    barrier = pltpu.get_barrier_semaphore()

    def greet(step, carry):
        pl.semaphore_signal(
            barrier,
            inc=1,
            device_id={"seq": lax.rem(me + step, groups)},
            device_id_type=MESH,
        )
        return carry

    lax.fori_loop(1, groups, greet, 0)

    lane = lax.broadcasted_iota(jnp.int32, (1, 128), 1)
    low = lane < 64
    inner = jnp.where(low, lane, lane - 64)
    even = inner < HALF

    row = lax.broadcasted_iota(jnp.int32, (TILE, 128), 0)
    column = lax.broadcasted_iota(jnp.int32, (TILE, 128), 1)
    ones = jnp.where((row < 128) == (column < 64), 1.0, 0.0).astype(jnp.bfloat16)
    for i in range(8):
        v_s[i, :, pl.ds(128, 128)] = ones
    embedded[pl.ds(bands * 32, (SLOTS - bands) * 32), :] = jnp.zeros(
        ((SLOTS - bands) * 32, D), jnp.bfloat16
    )

    def prepare(layer):
        for part in range(3):
            source = qkv_raw[layer, :, pl.ds(part * D, D)]
            spread = value_p[...] if part == 2 else rotary_p[...]
            qkv_w[layer, :, pl.ds(part * WIDE, WIDE)] = dot(source, spread).astype(
                jnp.bfloat16
            )
        mix_w[layer] = dot(spread_p[...], mix_raw[layer]).astype(jnp.bfloat16)

    for load in loads[:5]:
        load.wait()
    prepare(0)

    gain = gains[0:1, :]
    for i in range(lanes.shape[0]):
        lanes[i] = spectrum[:, pl.ds(128 * i, 128)]

    def embed(step, carry):
        for k in range(5):
            band = step * 5 + k
            start = table[band, 0]
            width = table[band, 1]
            block = lax.div(start, 128)
            offset = lax.rem(start, 128)
            window = jnp.concatenate([lanes[block], lanes[block + 1]], axis=1)
            first = pltpu.roll(window[0:32], lax.rem(256 - offset, 256), 1)[:, :128]
            second = pltpu.roll(window[32:64], lax.rem(320 - offset, 256), 1)[:, :128]
            picked = jnp.where(low, first, second)
            picked = jnp.where(inner < width, picked, 0.0).astype(jnp.bfloat16)
            rows = normalize(dot(picked, band_w[band]), gain)
            at = pl.multiple_of(band * 32, 32)
            embedded[pl.ds(at, 32), :] = rows.astype(jnp.bfloat16)
        return carry

    for i in range(4):
        loads[5 + i].wait()
        lax.fori_loop(i * 3, i * 3 + 3, embed, 0)
    for load in loads[9:]:
        load.wait()

    def turn_bands(step, carry):
        band_at = lax.rem(step, 4) * 16
        row_at = (step // 4) * 16
        block = jnp.concatenate(
            [
                embedded[pl.ds(pl.multiple_of((band_at + i) * 32 + row_at, 16), 16), :]
                for i in range(16)
            ],
            axis=0,
        )
        result = dot(swap_p[0], block).astype(jnp.bfloat16)
        for i in range(16):
            at = pl.multiple_of((row_at + i) * SLOTS + band_at, 16)
            stream[pl.ds(at, 16), :] = result[16 * i : 16 * i + 16]
        return carry

    lax.fori_loop(0, 8, turn_bands, 0)

    def sublayer(layer, x, mask):
        at = layer * 4
        first_gain = gains[1 + 2 * layer : 2 + 2 * layer, :]
        second_gain = gains[2 + 2 * layer : 3 + 2 * layer, :]
        xf = x.astype(jnp.float32)
        normed = normalize(xf, first_gain).astype(jnp.bfloat16)
        tables = [rope[at + i] for i in range(4)]
        for part in range(2):
            mixed = dot(normed, qkv_w[layer, :, pl.ds(part * WIDE, WIDE)])
            for r in range(2):
                for pair in range(4):
                    value = mixed[128 * r : 128 * r + 128, 128 * pair : 128 * pair + 128]
                    value = (
                        value * tables[2 * part]
                        + pltpu.roll(value, 64, 1) * tables[2 * part + 1]
                    )
                    if part == 0:
                        q_s[pl.ds(128 * r, 128), pl.ds(128 * pair, 128)] = value.astype(
                            jnp.bfloat16
                        )
                    else:
                        k_s[4 * r + pair, pl.ds(0, 128), :] = jnp.where(
                            even, value, 0.0
                        ).astype(jnp.bfloat16)
                        k_s[4 * r + pair, pl.ds(128, 128), :] = jnp.where(
                            even, 0.0, value
                        ).astype(jnp.bfloat16)
        mixed = dot(normed, qkv_w[layer, :, pl.ds(2 * WIDE, WIDE)])
        for r in range(2):
            for pair in range(4):
                value = mixed[128 * r : 128 * r + 128, 128 * pair : 128 * pair + 128]
                v_s[4 * r + pair, pl.ds(0, 128), pl.ds(0, 128)] = jnp.where(
                    low, value, 0.0
                ).astype(jnp.bfloat16)
                v_s[4 * r + pair, pl.ds(128, 128), pl.ds(0, 128)] = jnp.where(
                    low, 0.0, value
                ).astype(jnp.bfloat16)
        for r in range(2):
            for pair in range(4):
                scores = lax.dot_general(
                    q_s[pl.ds(128 * r, 128), pl.ds(128 * pair, 128)],
                    k_s[4 * r + pair],
                    (((1,), (1,)), ((), ())),
                    preferred_element_type=jnp.float32,
                )
                probs = []
                for head in range(2):
                    score = scores[:, 128 * head : 128 * head + 128]
                    if mask is not None:
                        score = jnp.where(mask, score, NEG)
                    score = score - jnp.max(score, axis=-1, keepdims=True)
                    probs.append(jnp.exp2(score).astype(jnp.bfloat16))
                both = dot(jnp.concatenate(probs, axis=1), v_s[4 * r + pair])
                c_s[pl.ds(128 * r, 128), pl.ds(128 * pair, 128)] = (
                    both[:, :128] / both[:, 128:]
                ).astype(jnp.bfloat16)
        x = (xf + dot(c_s[...], mix_w[layer])).astype(jnp.bfloat16)
        xf = x.astype(jnp.float32)
        normed = normalize(xf, second_gain).astype(jnp.bfloat16)
        active = jax.nn.gelu(dot(normed, ff_in[layer]), approximate=True).astype(
            jnp.bfloat16
        )
        return (xf + dot(active, ff_out[layer])).astype(jnp.bfloat16)

    def send(source, target, place, phase, half):
        at = pl.multiple_of(half * half_rows + target * CHUNK, CHUNK)
        to = pl.multiple_of(half * half_rows + me * CHUNK, CHUNK)

        @pl.when(target != me)
        def _():
            pltpu.make_async_remote_copy(
                src_ref=source.at[pl.ds(at, CHUNK)],
                dst_ref=place.at[pl.ds(to, CHUNK)],
                send_sem=send_sem.at[2 * phase + half],
                recv_sem=recv_sem.at[2 * phase + half],
                device_id={"seq": target},
                device_id_type=MESH,
            ).start()

        @pl.when(target == me)
        def _():
            pltpu.make_async_copy(
                source.at[pl.ds(at, CHUNK)],
                place.at[pl.ds(to, CHUNK)],
                recv_sem.at[2 * phase + half],
            ).start()

    query_at = lax.broadcasted_iota(jnp.int32, (128, 128), 0)
    key_at = lax.broadcasted_iota(jnp.int32, (128, 128), 1)
    key_band = jnp.where(key_at < SLOTS, key_at, key_at - SLOTS)
    band_mask = ((query_at < SLOTS) == (key_at < SLOTS)) & (key_band < bands)

    own = me // (groups // 4)

    def band_step(step, carry):
        half = step // 4
        block = half * 4 + lax.rem(step + own, 4)
        at = pl.multiple_of(block * TILE, TILE)
        stream[pl.ds(at, TILE), :] = sublayer(0, stream[pl.ds(at, TILE), :], band_mask)

        @pl.when(step == 0)
        def _():
            pl.semaphore_wait(barrier, groups - 1)

        def post(i, inner_carry):
            target = lax.rem(step + own, 4) * 32 + lax.rem(me + i, 32)
            send(stream, target, arrived, 0, half)
            return inner_carry

        lax.fori_loop(0, 32, post, 0)
        return carry

    lax.fori_loop(0, 8, band_step, 0)
    prepare(1)

    def time_half(half, carry):
        base = pl.multiple_of(half * half_rows, half_rows)
        whole = arrived.at[pl.ds(base, half_rows)]
        pltpu.make_async_copy(whole, whole, recv_sem.at[half]).wait()
        for k in range(4):
            block = arrived[pl.ds(base + k * TILE, TILE), :]
            result = dot(swap_p[1], block).astype(jnp.bfloat16)
            for i in range(8):
                turned[pl.ds(i * 128 + 32 * k, 32), :] = result[32 * i : 32 * i + 32]

        def time_step(step, inner_carry):
            at = pl.multiple_of(step * TILE, TILE)
            x = sublayer(1, turned[pl.ds(at, TILE), :], None)
            hidden[pl.ds(at, TILE), :] = normalize(
                x.astype(jnp.float32), gains[5:6, :]
            ).astype(jnp.bfloat16)
            return inner_carry

        lax.fori_loop(0, 4, time_step, 0)
        for k in range(4):
            block = jnp.concatenate(
                [hidden[pl.ds(i * 128 + 32 * k, 32), :] for i in range(8)], axis=0
            )
            leaving[pl.ds(base + k * TILE, TILE), :] = dot(swap_p[2], block).astype(
                jnp.bfloat16
            )

        def post(i, inner_carry):
            send(leaving, lax.rem(me + i, groups), out_ref, 1, half)
            return inner_carry

        lax.fori_loop(0, groups, post, 0)
        return carry

    lax.fori_loop(0, 2, time_half, 0)
    for half in range(2):
        whole = out_ref.at[pl.ds(half * half_rows, half_rows)]
        pltpu.make_async_copy(whole, whole, recv_sem.at[2 + half]).wait()
    for i in range(4):
        sent = stream.at[pl.ds(0, half_rows - CHUNK)]
        pltpu.make_async_copy(sent, sent, send_sem.at[i]).wait()


def body(
    spectrum,
    band_table,
    band_weight,
    qkv_weight,
    out_weight,
    ff_in_weight,
    ff_out_weight,
    norm_gains,
):
    _, batch, channels, bins = spectrum.shape
    bands = band_table.shape[0]
    hidden_size = ff_in_weight.shape[-1]
    groups = lax.axis_size("seq")
    rotary, value = head_columns()
    band_positions = np.arange(128) % SLOTS
    rope = np.stack(rotary_tables(band_positions) + rotary_tables(np.arange(128)))
    swaps = np.stack([swap_matrix(16, 16), swap_matrix(32, 8), swap_matrix(8, 32)])
    rows = batch * SLOTS
    flat = jnp.swapaxes(spectrum[0], 0, 1).reshape(channels * batch, bins)
    flat = jnp.pad(flat.astype(jnp.float32), ((0, 0), (0, 1152 - bins)))
    bf16 = jnp.bfloat16
    hbm = pl.BlockSpec(memory_space=pl.ANY)
    vmem = pl.BlockSpec(memory_space=pltpu.VMEM)
    result = pl.pallas_call(
        functools.partial(kernel, groups, bands),
        out_shape=jax.ShapeDtypeStruct((rows, D), bf16),
        in_specs=[pl.BlockSpec(memory_space=pltpu.SMEM), vmem, vmem] + [hbm] * 10,
        out_specs=vmem,
        scratch_shapes=[
            pltpu.VMEM((bands, channels * SPAN, D), bf16),
            pltpu.VMEM((2, D, 3 * D), bf16),
            pltpu.VMEM((2, D, D), bf16),
            pltpu.VMEM((2, D, hidden_size), bf16),
            pltpu.VMEM((2, hidden_size, D), bf16),
            pltpu.VMEM((8, 128, 128), jnp.float32),
            pltpu.VMEM((D, WIDE), bf16),
            pltpu.VMEM((D, WIDE), bf16),
            pltpu.VMEM((WIDE, D), bf16),
            pltpu.VMEM((3, TILE, TILE), bf16),
            pltpu.VMEM((2, D, 3 * WIDE), bf16),
            pltpu.VMEM((2, WIDE, D), bf16),
            pltpu.VMEM((rows, D), bf16),
            pltpu.VMEM((rows, D), bf16),
            pltpu.VMEM((rows, D), bf16),
            pltpu.VMEM((rows // 2, D), bf16),
            pltpu.VMEM((rows // 2, D), bf16),
            pltpu.VMEM((rows, D), bf16),
            pltpu.VMEM((TILE, WIDE), bf16),
            pltpu.VMEM((8, TILE, 128), bf16),
            pltpu.VMEM((8, TILE, 256), bf16),
            pltpu.VMEM((TILE, WIDE), bf16),
            pltpu.VMEM((9, channels * batch, 128), jnp.float32),
            pltpu.SemaphoreType.DMA((13,)),
            pltpu.SemaphoreType.DMA((4,)),
            pltpu.SemaphoreType.DMA((4,)),
        ],
        compiler_params=pltpu.CompilerParams(
            collective_id=0, has_side_effects=True, vmem_limit_bytes=60 * 1024 * 1024
        ),
    )(
        band_table,
        flat,
        norm_gains,
        band_weight.reshape(bands, channels * SPAN, D),
        qkv_weight,
        out_weight,
        ff_in_weight,
        ff_out_weight,
        jnp.asarray(rope, jnp.float32),
        jnp.asarray(rotary, bf16),
        jnp.asarray(value, bf16),
        jnp.asarray(value.T, bf16),
        jnp.asarray(swaps, bf16),
    )
    return result.reshape(1, batch, SLOTS, D)[:, :, :bands]


def solution(mesh):
    in_specs = (P("seq", "dp", None, None), P(), P(), P(), P(), P(), P(), P())
    out_specs = P("seq", "dp", None, None)
    return jax.shard_map(body, mesh=mesh, in_specs=in_specs, out_specs=out_specs, check_vma=False)
```
